32 devices in a mesh: dp: 8 (over z, y), mp: 4 (over x, core).
Axes of the slice: x: 2, y: 2, z: 4, core: 2. Of those that a mesh axis runs over, the one named last changes fastest.
Arguments:
- gradients: bfloat16 [4, 16, 1024, 1024], P(None, 'mp', 'dp'), as said below
- statistics: float32 [4, 32, 1024, 1024], P('mp', 'dp'), as said below
- accumulator: float32 [4, 16, 1024, 1024], P(None, 'mp', 'dp'), may hold values from 0.25 to 4
Outputs:
- update: float32 [4, 16, 1024, 1024], P(None, 'mp', 'dp')
- statistics_new: float32 [4, 32, 1024, 1024], P('mp', 'dp')
- accumulator_new: float32 [4, 16, 1024, 1024], P(None, 'mp', 'dp')
The draws below stay inside these ranges and needn't reach their ends.
Inputs may be any that keep to these rules, and one draw needn't show every extreme that they name: `gradients`: Real-valued gradient blocks. `statistics`: each 1024 x 1024 statistic is symmetric positive definite.
All inputs are finite; a program needn't handle non-finite values.
Results may differ from the reference program's by a relative error of at most 0.005.
The reference program's roundings to bfloat16 on the way count: a program that leaves them out, or rounds other values in their place, can miss the bound.
Values may be sent and summed in bfloat16 or wider, within the bound.
No kernel may reach another device: no remote copies, remote signals or barrier semaphores. Data moves between devices by JAX's collectives and lax.ppermute only.
A program may use at most 192 MiB of HBM per device.

```python
import math
import jax
import jax.numpy as jnp
from jax import lax

B = 1024
ITERS = 3
RB = 4
CB = 16
CB_MP = 4
BLKS = 16
N_MP = 4


def draw_gradients(key, part):
    subkeys = jax.random.split(key, 3)
    gaussian = jax.random.normal(subkeys[0], (RB, CB, B, B), jnp.float32)
    row_scale = 10.0 ** jax.random.uniform(subkeys[1], (RB, CB, B, 1), jnp.float32)
    col_scale = 10.0 ** jax.random.uniform(subkeys[2], (RB, CB, 1, B), jnp.float32)
    rising = (3.0 ** (jnp.arange(B, dtype=jnp.float32) / B))[:, None]
    values = gaussian * row_scale * col_scale * rising
    return values.astype(jnp.bfloat16)


def draw_statistics(key, part):
    spread = 2.0

    def one_matrix(position):
        matrix_key = jax.random.fold_in(key, position)
        noise_key, scale_key = jax.random.split(matrix_key)
        gaussian = jax.random.normal(noise_key, (B, B), jnp.float32)
        wishart = jnp.dot(gaussian, gaussian.T, precision=lax.Precision.HIGHEST) / B + 0.5 * jnp.eye(B, dtype=jnp.float32)
        diagonal_scale = jnp.exp(jax.random.uniform(scale_key, (B,), jnp.float32) * jnp.log(spread))
        return 0.25 * diagonal_scale[:, None] * wishart * diagonal_scale[None, :]
    matrices = lax.map(one_matrix, jnp.arange(N_MP * 2 * BLKS, dtype=jnp.int32))
    return matrices.reshape(N_MP, 2 * BLKS, B, B)


def shard_levels(own_key, extent, cuts, smallest, high):
    def one(dim, blocks):
        heights = jax.random.uniform(jax.random.fold_in(jax.random.fold_in(own_key, 6), dim), (blocks,), jnp.float32, smallest / len(cuts), high / len(cuts))
        return jnp.repeat(jnp.exp(heights), extent[dim] // blocks).reshape((-1,) + (1,) * (len(extent) - dim - 1))

    factor_of = one(*cuts[0])
    for cut in cuts[1:]:
        factor_of = factor_of * one(*cut)
    return factor_of


def setup_inputs(seed: int = 0) -> dict:
    streams_of = jax.random.split(jax.random.key(seed), 4)
    gradients = draw_gradients(jax.random.fold_in(streams_of[3], 71), 0)
    statistics = draw_statistics(jax.random.fold_in(streams_of[3], 71), 0)
    accumulator = jnp.clip(jnp.exp(math.log(4.0) - 2.7725887 * jax.random.uniform(streams_of[2], (RB, CB, B, B), jnp.float32) ** shard_levels(streams_of[2], (RB, CB, B, B), ((1, 4), (2, 8)), -0.2, 0.2)), 0.25, 4.0)
    return {"gradients": gradients, "statistics": statistics, "accumulator": accumulator}


def matmul(left, right):
    return jnp.dot(left.astype(jnp.float32), right.astype(jnp.float32), precision=lax.Precision.HIGHEST)

def inverse_root(statistic):
    identity = jnp.eye(statistic.shape[0], dtype=jnp.float32)
    frob_norm = jnp.sqrt(jnp.sum(statistic * statistic) + 1e-06)
    newton_scale = 2.5 / frob_norm
    matrix = newton_scale * statistic
    root_iter = jnp.sqrt(jnp.sqrt(newton_scale)) * identity
    for iteration in range(ITERS):
        factor = (1.25 * identity - 0.25 * matrix).astype(jnp.bfloat16)
        root_iter = matmul(root_iter.astype(jnp.bfloat16), factor)
        if iteration + 1 < ITERS:
            square = matmul(factor, factor).astype(jnp.bfloat16)
            fourth = matmul(square, square).astype(jnp.bfloat16)
            matrix = matmul(fourth, matrix.astype(jnp.bfloat16))
    return root_iter

def reference(gradients, statistics, accumulator):
    grads_wide = gradients.astype(jnp.float32)
    grad_total = jnp.sum(grads_wide * grads_wide)
    clip_factor = jnp.minimum(1.0, jnp.sqrt(RB * CB * B * B / (grad_total + 1e-06)))

    def one_block(position):
        mp_shard = position // BLKS
        local_block = position % BLKS
        row_block = (local_block // CB_MP).astype(jnp.int32)
        col_block = (mp_shard * CB_MP + local_block % CB_MP).astype(jnp.int32)
        zero_index = jnp.zeros((), jnp.int32)
        grad_block = lax.dynamic_slice(gradients, (row_block, col_block, zero_index, zero_index), (1, 1, B, B))[0, 0]
        stat_pair = lax.dynamic_slice(statistics, (mp_shard.astype(jnp.int32), (2 * local_block).astype(jnp.int32), zero_index, zero_index), (1, 2, B, B))[0]
        left_stat = 0.9 * stat_pair[0] + 0.1 / B * clip_factor * clip_factor * matmul(grad_block, grad_block.T)
        right_stat = 0.9 * stat_pair[1] + 0.1 / B * clip_factor * clip_factor * matmul(grad_block.T, grad_block)
        left_root = inverse_root(left_stat).astype(jnp.bfloat16)
        right_root = inverse_root(right_stat).astype(jnp.bfloat16)
        left_applied = matmul(left_root, grad_block).astype(jnp.bfloat16)
        product = matmul(left_applied, right_root)
        return (jnp.stack([left_stat, right_stat]), product)
    stats_all, products = lax.map(one_block, jnp.arange(N_MP * BLKS, dtype=jnp.int32))
    statistics_new = stats_all.reshape(N_MP, 2 * BLKS, B, B)
    preconditioned = products.reshape(N_MP, RB, CB_MP, B, B).transpose(1, 0, 2, 3, 4).reshape(RB, CB, B, B)
    scaled = clip_factor * grads_wide
    accumulated = accumulator + scaled * scaled
    graft_step = scaled / jnp.sqrt(accumulated)
    graft_ratio = jnp.sqrt(jnp.sum(graft_step * graft_step) / (jnp.sum(preconditioned * preconditioned) + 1e-06))
    return (graft_ratio * preconditioned, statistics_new, accumulated)
```

```python
import functools

import jax
import jax.numpy as jnp
from jax import lax
from jax.experimental import pallas as pl
from jax.experimental.pallas import tpu as pltpu
from jax.sharding import PartitionSpec as P


ITERS = 3
PANEL = 256


def partner_2(value, axis, distance):
    return lax.ppermute(value, axis, [(i, i ^ 1 << distance) for i in range(lax.axis_size(axis))])


def batch_dot(left, right):
    return jnp.einsum("kij,kjl->kil", left, right, preferred_element_type=jnp.float32)


def inverse_roots(statistic):
    block_width = statistic.shape[-1]
    identity = jnp.eye(block_width, dtype=jnp.float32)
    frob_norms = jnp.sqrt(jnp.sum(statistic * statistic, axis=(1, 2)) + 1e-06)
    newton_scale = (2.5 / frob_norms)[:, None, None]
    matrix = newton_scale * statistic
    root_iter = jnp.sqrt(jnp.sqrt(newton_scale)) * identity
    for iteration in range(ITERS):
        factor = (1.25 * identity - 0.25 * matrix).astype(jnp.bfloat16)
        root_iter = batch_dot(root_iter.astype(jnp.bfloat16), factor)
        if iteration + 1 < ITERS:
            square = batch_dot(factor, factor).astype(jnp.bfloat16)
            fourth = batch_dot(square, square).astype(jnp.bfloat16)
            matrix = batch_dot(fourth, matrix.astype(jnp.bfloat16))
    return root_iter


def on_device_plain(gradients, statistics, accumulator):
    owners = lax.axis_size("dp")
    own_index = lax.axis_index("dp")
    row_blocks, col_blocks, dev_rows, block_width = gradients.shape
    blocks = row_blocks * col_blocks
    owned_factors = statistics.shape[1]
    split_pairs = owned_factors == 1
    half_rows = dev_rows // 2
    parity = own_index % 2
    left_side = parity == 0
    by_block = gradients.reshape(blocks, dev_rows, block_width)
    grads_wide = gradients.astype(jnp.float32)
    grad_total = lax.psum(jnp.sum(grads_wide * grads_wide), ("dp", "mp"))
    entries = blocks * dev_rows * block_width * owners * lax.axis_size("mp")
    clip_factor = jnp.minimum(1.0, jnp.sqrt(entries / (grad_total + 1e-06)))
    scaled = clip_factor * grads_wide
    accumulated = accumulator + scaled * scaled
    graft_step = scaled / jnp.sqrt(accumulated)
    graft_squares = jnp.sum(graft_step * graft_step)
    row_parts = 2 if split_pairs else 1
    row_units = by_block.reshape(blocks * row_parts, dev_rows // row_parts, block_width)
    received = lax.all_to_all(row_units, "dp", split_axis=0, concat_axis=1, tiled=True)
    if split_pairs:
        partner_part = partner_2(received, "dp", 0)
        own_part = received.reshape(owners, 1, half_rows, block_width)
        partner_part = partner_part.reshape(owners, 1, half_rows, block_width)
        ordered = jnp.where(
            left_side,
            jnp.concatenate([own_part, partner_part], 1),
            jnp.concatenate([partner_part, own_part], 1),
        )
        whole_blocks = ordered.reshape(1, owners * dev_rows, block_width)
    else:
        whole_blocks = received
    transposed = jnp.swapaxes(whole_blocks, 1, 2)
    if split_pairs:
        factor_inputs = jnp.where(left_side, whole_blocks, transposed)
    else:
        factor_inputs = jnp.stack([whole_blocks, transposed], 1).reshape(
            owned_factors, block_width, block_width
        )
    gram_matrix = jnp.einsum(
        "kij,klj->kil", factor_inputs, factor_inputs, preferred_element_type=jnp.float32
    )
    statistics_new = (
        0.9 * statistics[0] + 0.1 / block_width * clip_factor * clip_factor * gram_matrix
    )
    root_values = inverse_roots(statistics_new).astype(jnp.bfloat16)
    if split_pairs:
        partner = partner_2(root_values, "dp", 0)
        left_root = jnp.where(left_side, root_values, partner)[0]
        right_root = jnp.where(left_side, partner, root_values)[0]
        left_rows = lax.dynamic_slice_in_dim(
            left_root.reshape(owners, 2, half_rows, block_width), parity, 1, 1
        )
        left_rows = left_rows.reshape(owners * half_rows, block_width)
        left_applied = jnp.dot(
            left_rows, whole_blocks[0], preferred_element_type=jnp.float32
        ).astype(jnp.bfloat16)
        product = jnp.dot(left_applied, right_root, preferred_element_type=jnp.float32)
        pieces = product.reshape(1, owners, half_rows, block_width)
    else:
        root_pairs = root_values.reshape(-1, 2, block_width, block_width)
        left_applied = batch_dot(root_pairs[:, 0], whole_blocks).astype(jnp.bfloat16)
        product = batch_dot(left_applied, root_pairs[:, 1])
        pieces = product.reshape(-1, owners, dev_rows, block_width)
    returned = lax.all_to_all(
        pieces.astype(jnp.bfloat16), "dp", split_axis=1, concat_axis=0, tiled=True
    ).astype(pieces.dtype)
    returned = returned.reshape(row_blocks, col_blocks, dev_rows, block_width)
    graft_total, update_total = lax.psum(
        (graft_squares, jnp.sum(returned * returned)), ("dp", "mp")
    )
    graft_ratio = jnp.sqrt(graft_total / (update_total + 1e-06))
    return (graft_ratio * returned, statistics_new[None], accumulated)


def eye_tile(n):
    rows = lax.broadcasted_iota(jnp.int32, (n, n), 0)
    cols = lax.broadcasted_iota(jnp.int32, (n, n), 1)
    return rows == cols


def dot_f32(left, right):
    return jnp.dot(left, right, preferred_element_type=jnp.float32)


def panels(width):
    return [(start, start + PANEL) for start in range(0, width, PANEL)]


def store_symmetric(ref, upper, start, stop):
    ref[:stop, start:stop] = upper
    if start:
        ref[start:stop, :start] = upper[:start].T


def block_kernel(block, scale_ref, grad_hbm, stat_hbm, *rest):
    (stat_out, prod_out, squares_out,
     grad, grad_t, stat, mats, facs, roots, square, fourth, prod,
     sem_g, sem_s, sem_o, sem_p) = rest[-16:]
    width = grad.shape[0]
    grad_in = pltpu.make_async_copy(grad_hbm, grad, sem_g)
    grad_in.start()
    stat_in = [pltpu.make_async_copy(stat_hbm.at[2 * block + s], stat.at[s], sem_s.at[s]) for s in range(2)]
    for copy in stat_in:
        copy.start()
    grad_in.wait()
    scale = scale_ref[0]
    grad_t[...] = grad[...].T
    frob = []
    stat_done = []
    for s, (left, right) in enumerate(((grad, grad_t), (grad_t, grad))):
        stat_in[s].wait()
        total = jnp.zeros((1, 1), jnp.float32)
        for start, stop in panels(width):
            gram = scale * dot_f32(left[:stop, :], right[:, start:stop])
            upper = 0.9 * stat[s, :stop, start:stop] + gram
            stat[s, :stop, start:stop] = upper
            diag = upper[start:]
            total = total + jnp.sum(diag * diag, keepdims=True)
            if start:
                lower = 0.9 * stat[s, start:stop, :start] + gram[:start].T
                stat[s, start:stop, :start] = lower
                total = total + jnp.sum(upper[:start] * upper[:start], keepdims=True)
                total = total + jnp.sum(lower * lower, keepdims=True)
        copy = pltpu.make_async_copy(stat.at[s], stat_out.at[2 * block + s], sem_o.at[s])
        copy.start()
        stat_done.append(copy)
        frob.append(jnp.sqrt(total + 1e-06))
    eye = eye_tile(PANEL)
    for s in range(2):
        z = 2.5 / frob[s]
        root0 = jnp.sqrt(jnp.sqrt(z)).astype(jnp.bfloat16).astype(jnp.float32)
        for start, stop in panels(width):
            for low, high in panels(width):
                matrix = z * stat[s, low:high, start:stop]
                factor = -0.25 * matrix
                if low == start:
                    factor = jnp.where(eye, 1.25, 0.0) + factor
                factor = factor.astype(jnp.bfloat16)
                mats[0, low:high, start:stop] = matrix.astype(jnp.bfloat16)
                facs[0, low:high, start:stop] = factor
                roots[s, 0, low:high, start:stop] = (root0 * factor.astype(jnp.float32)).astype(jnp.bfloat16)

        def newton(it, carry):
            cur, nxt = it, 1 - it
            for start, stop in panels(width):
                upper = dot_f32(facs[cur, :stop, :], facs[cur, :, start:stop])
                store_symmetric(square, upper.astype(jnp.bfloat16), start, stop)
            for start, stop in panels(width):
                upper = dot_f32(square[:stop, :], square[:, start:stop])
                store_symmetric(fourth, upper.astype(jnp.bfloat16), start, stop)
            for start, stop in panels(width):
                upper = dot_f32(fourth[:stop, :], mats[cur, :, start:stop])
                store_symmetric(mats.at[nxt], upper.astype(jnp.bfloat16), start, stop)
                diag = jnp.where(eye, 1.25, 0.0) - 0.25 * upper[start:]
                facs[nxt, start:stop, start:stop] = diag.astype(jnp.bfloat16)
                if start:
                    off = (-0.25 * upper[:start]).astype(jnp.bfloat16)
                    facs[nxt, :start, start:stop] = off
                    facs[nxt, start:stop, :start] = off.T
            for start, stop in panels(width):
                upper = dot_f32(roots[s, cur, :stop, :], facs[nxt, :, start:stop])
                store_symmetric(roots.at[s, nxt], upper.astype(jnp.bfloat16), start, stop)
            return carry

        lax.fori_loop(0, ITERS - 1, newton, 0)
    last = (ITERS - 1) % 2
    applied = square
    for start, stop in panels(width):
        applied[:, start:stop] = dot_f32(roots[0, last], grad[:, start:stop]).astype(jnp.bfloat16)
    squares = jnp.zeros((1, 1), jnp.float32)
    for start, stop in panels(width):
        value = dot_f32(applied[...], roots[1, last, :, start:stop])
        prod[:, start:stop] = value.astype(jnp.bfloat16)
        squares = squares + jnp.sum(value * value, keepdims=True)
    send = pltpu.make_async_copy(prod, prod_out, sem_p)
    send.start()
    squares_out[...] = jnp.broadcast_to(squares, squares_out.shape)
    for copy in stat_done:
        copy.wait()
    send.wait()


def block_call(block, scale, grad, statistics, carried):
    width = grad.shape[-1]
    square = (width, width)
    any_spec = pl.BlockSpec(memory_space=pl.ANY)
    operands = [scale, grad, statistics]
    in_specs = [pl.BlockSpec(memory_space=pltpu.SMEM), any_spec, any_spec]
    aliases = {}
    if carried is not None:
        aliases = {len(operands): 0}
        operands.append(carried)
        in_specs.append(any_spec)
    flops = 2 * width ** 3 * 16
    return pl.pallas_call(
        functools.partial(block_kernel, block),
        out_shape=(
            jax.ShapeDtypeStruct(statistics.shape, jnp.float32),
            jax.ShapeDtypeStruct(square, jnp.bfloat16),
            jax.ShapeDtypeStruct((1, 128), jnp.float32),
        ),
        in_specs=in_specs,
        out_specs=(any_spec, any_spec, pl.BlockSpec(memory_space=pltpu.VMEM)),
        scratch_shapes=[
            pltpu.VMEM(square, jnp.bfloat16),
            pltpu.VMEM(square, jnp.bfloat16),
            pltpu.VMEM((2,) + square, jnp.float32),
            pltpu.VMEM((2,) + square, jnp.bfloat16),
            pltpu.VMEM((2,) + square, jnp.bfloat16),
            pltpu.VMEM((2, 2) + square, jnp.bfloat16),
            pltpu.VMEM(square, jnp.bfloat16),
            pltpu.VMEM(square, jnp.bfloat16),
            pltpu.VMEM(square, jnp.bfloat16),
            pltpu.SemaphoreType.DMA,
            pltpu.SemaphoreType.DMA((2,)),
            pltpu.SemaphoreType.DMA((2,)),
            pltpu.SemaphoreType.DMA,
        ],
        input_output_aliases=aliases,
        compiler_params=pltpu.CompilerParams(vmem_limit_bytes=56 * 1024 * 1024),
        cost_estimate=pl.CostEstimate(flops=flops, bytes_accessed=20 * width * width, transcendentals=0),
    )(*operands)


def sum_everywhere(value, axes):
    for axis in axes:
        size = lax.axis_size(axis)
        distance = 1
        while distance < size:
            value = value + lax.ppermute(value, axis, [(i, i ^ distance) for i in range(size)])
            distance *= 2
    return value


def exchange(pieces):
    return lax.all_to_all(pieces, "dp", split_axis=0, concat_axis=0, tiled=True)


def on_device(gradients, statistics, accumulator):
    owners = lax.axis_size("dp")
    row_blocks, col_blocks, dev_rows, block_width = gradients.shape
    blocks = row_blocks * col_blocks
    chunks = statistics.shape[1] // 2
    by_owner = gradients.reshape(owners, chunks, dev_rows, block_width)
    grads_wide = gradients.astype(jnp.float32)
    squares = jnp.full((1, 128), jnp.sum(grads_wide * grads_wide))
    grad_total = sum_everywhere(squares, ("mp", "dp"))[0, 0]
    entries = blocks * dev_rows * block_width * owners * lax.axis_size("mp")
    clip_factor = jnp.minimum(1.0, jnp.sqrt(entries / (grad_total + 1e-06)))
    scale = (0.1 / block_width * clip_factor * clip_factor).reshape(1)
    wholes = []
    for c in range(chunks):
        whole = exchange(by_owner[:, c])
        wholes.append(whole.reshape(block_width, block_width))
    scaled = clip_factor * grads_wide
    accumulated = accumulator + scaled * scaled
    graft_step = scaled / jnp.sqrt(accumulated)
    graft_squares = jnp.sum(graft_step * graft_step)
    statistics_new = None
    returned = []
    update_squares = jnp.zeros((1, 128), jnp.float32)
    for c in range(chunks):
        statistics_new, product, part = block_call(c, scale, wholes[c], statistics[0], statistics_new)
        update_squares = update_squares + part
        returned.append(exchange(product.reshape(owners, dev_rows, block_width)))
    lanes = lax.broadcasted_iota(jnp.int32, (1, 128), 1)
    sums = jnp.where(lanes == 0, graft_squares, update_squares)
    sums = sum_everywhere(sums, ("mp", "dp"))
    graft_ratio = jnp.sqrt(sums[0, 0] / (sums[0, 1] + 1e-06))
    update = graft_ratio * jnp.stack(returned, 1).astype(jnp.float32)
    update = update.reshape(gradients.shape)
    return (update, statistics_new[None], accumulated)


def solution(mesh):
    def run(gradients, statistics, accumulator):
        if statistics.shape[1] % 2:
            return on_device_plain(gradients, statistics, accumulator)
        return on_device(gradients, statistics, accumulator)

    return jax.shard_map(
        run,
        mesh=mesh,
        in_specs=(P(None, "mp", "dp", None), P("mp", "dp", None, None), P(None, "mp", "dp", None)),
        out_specs=(P(None, "mp", "dp", None), P("mp", "dp", None, None), P(None, "mp", "dp", None)),
        check_vma=False,
    )
```

```python
import functools

import jax
import jax.numpy as jnp
from jax import lax
from jax.experimental import pallas as pl
from jax.experimental.pallas import tpu as pltpu
from jax.sharding import PartitionSpec as P


ITERS = 3
PANEL = 256


def partner_2(value, axis, distance):
    return lax.ppermute(value, axis, [(i, i ^ 1 << distance) for i in range(lax.axis_size(axis))])


def batch_dot(left, right):
    return jnp.einsum("kij,kjl->kil", left, right, preferred_element_type=jnp.float32)


def inverse_roots(statistic):
    block_width = statistic.shape[-1]
    identity = jnp.eye(block_width, dtype=jnp.float32)
    frob_norms = jnp.sqrt(jnp.sum(statistic * statistic, axis=(1, 2)) + 1e-06)
    newton_scale = (2.5 / frob_norms)[:, None, None]
    matrix = newton_scale * statistic
    root_iter = jnp.sqrt(jnp.sqrt(newton_scale)) * identity
    for iteration in range(ITERS):
        factor = (1.25 * identity - 0.25 * matrix).astype(jnp.bfloat16)
        root_iter = batch_dot(root_iter.astype(jnp.bfloat16), factor)
        if iteration + 1 < ITERS:
            square = batch_dot(factor, factor).astype(jnp.bfloat16)
            fourth = batch_dot(square, square).astype(jnp.bfloat16)
            matrix = batch_dot(fourth, matrix.astype(jnp.bfloat16))
    return root_iter


def on_device_plain(gradients, statistics, accumulator):
    owners = lax.axis_size("dp")
    own_index = lax.axis_index("dp")
    row_blocks, col_blocks, dev_rows, block_width = gradients.shape
    blocks = row_blocks * col_blocks
    owned_factors = statistics.shape[1]
    split_pairs = owned_factors == 1
    half_rows = dev_rows // 2
    parity = own_index % 2
    left_side = parity == 0
    by_block = gradients.reshape(blocks, dev_rows, block_width)
    grads_wide = gradients.astype(jnp.float32)
    grad_total = lax.psum(jnp.sum(grads_wide * grads_wide), ("dp", "mp"))
    entries = blocks * dev_rows * block_width * owners * lax.axis_size("mp")
    clip_factor = jnp.minimum(1.0, jnp.sqrt(entries / (grad_total + 1e-06)))
    scaled = clip_factor * grads_wide
    accumulated = accumulator + scaled * scaled
    graft_step = scaled / jnp.sqrt(accumulated)
    graft_squares = jnp.sum(graft_step * graft_step)
    row_parts = 2 if split_pairs else 1
    row_units = by_block.reshape(blocks * row_parts, dev_rows // row_parts, block_width)
    received = lax.all_to_all(row_units, "dp", split_axis=0, concat_axis=1, tiled=True)
    if split_pairs:
        partner_part = partner_2(received, "dp", 0)
        own_part = received.reshape(owners, 1, half_rows, block_width)
        partner_part = partner_part.reshape(owners, 1, half_rows, block_width)
        ordered = jnp.where(
            left_side,
            jnp.concatenate([own_part, partner_part], 1),
            jnp.concatenate([partner_part, own_part], 1),
        )
        whole_blocks = ordered.reshape(1, owners * dev_rows, block_width)
    else:
        whole_blocks = received
    transposed = jnp.swapaxes(whole_blocks, 1, 2)
    if split_pairs:
        factor_inputs = jnp.where(left_side, whole_blocks, transposed)
    else:
        factor_inputs = jnp.stack([whole_blocks, transposed], 1).reshape(
            owned_factors, block_width, block_width
        )
    gram_matrix = jnp.einsum(
        "kij,klj->kil", factor_inputs, factor_inputs, preferred_element_type=jnp.float32
    )
    statistics_new = (
        0.9 * statistics[0] + 0.1 / block_width * clip_factor * clip_factor * gram_matrix
    )
    root_values = inverse_roots(statistics_new).astype(jnp.bfloat16)
    if split_pairs:
        partner = partner_2(root_values, "dp", 0)
        left_root = jnp.where(left_side, root_values, partner)[0]
        right_root = jnp.where(left_side, partner, root_values)[0]
        left_rows = lax.dynamic_slice_in_dim(
            left_root.reshape(owners, 2, half_rows, block_width), parity, 1, 1
        )
        left_rows = left_rows.reshape(owners * half_rows, block_width)
        left_applied = jnp.dot(
            left_rows, whole_blocks[0], preferred_element_type=jnp.float32
        ).astype(jnp.bfloat16)
        product = jnp.dot(left_applied, right_root, preferred_element_type=jnp.float32)
        pieces = product.reshape(1, owners, half_rows, block_width)
    else:
        root_pairs = root_values.reshape(-1, 2, block_width, block_width)
        left_applied = batch_dot(root_pairs[:, 0], whole_blocks).astype(jnp.bfloat16)
        product = batch_dot(left_applied, root_pairs[:, 1])
        pieces = product.reshape(-1, owners, dev_rows, block_width)
    returned = lax.all_to_all(
        pieces.astype(jnp.bfloat16), "dp", split_axis=1, concat_axis=0, tiled=True
    ).astype(pieces.dtype)
    returned = returned.reshape(row_blocks, col_blocks, dev_rows, block_width)
    graft_total, update_total = lax.psum(
        (graft_squares, jnp.sum(returned * returned)), ("dp", "mp")
    )
    graft_ratio = jnp.sqrt(graft_total / (update_total + 1e-06))
    return (graft_ratio * returned, statistics_new[None], accumulated)


def dot_f32(left, right):
    return jnp.dot(left, right, preferred_element_type=jnp.float32)


def panels(width):
    return [(start, start + PANEL) for start in range(0, width, PANEL)]


def lane_sums(value):
    return jnp.sum(value.reshape(-1, 8, value.shape[-1]), axis=0)


def mirrored(left, right, out, post=None):
    for start, stop in panels(left.shape[0]):
        value = dot_f32(left[:stop, :], right[:, start:stop])
        upper = value.astype(jnp.bfloat16)
        out[:stop, start:stop] = upper
        if start:
            out[start:stop, :start] = upper[:start].T
        if post is not None:
            post(value, start, stop)


def block_kernel(block, partners, whole, me_ref, scale_ref, own_hbm, stat_hbm, *rest):
    received = rest[: len(partners)]
    outs = rest[len(rest) - 17 - (0 if whole else len(partners)):]
    stat_out = outs[0]
    prod_outs = outs[1 : len(outs) - 15]
    (squares_out,
     grads, stat_old, stat, matrix, factor, root, square, fourth, left_root, sums,
     sem_g, sem_s, sem_o, sem_p) = outs[len(outs) - 15:]
    width = grads.shape[1]
    dev_rows = own_hbm.shape[2]
    me = me_ref[0]

    def rows_of(partner):
        return pl.ds(pl.multiple_of((me ^ partner) * dev_rows, dev_rows), dev_rows)

    grad_in = [pltpu.make_async_copy(own_hbm.at[me, block], grads.at[0, rows_of(0), :], sem_g.at[0])]
    for n, partner in enumerate(partners):
        grad_in.append(pltpu.make_async_copy(received[n], grads.at[0, rows_of(partner), :], sem_g.at[n + 1]))
    for copy in grad_in:
        copy.start()
    stat_in = pltpu.make_async_copy(stat_hbm.at[pl.ds(2 * block, 2)], stat_old, sem_s)
    stat_in.start()
    for copy in grad_in:
        copy.wait()
    scale = scale_ref[0]
    tile = (PANEL, PANEL)
    eye = lax.broadcasted_iota(jnp.int32, tile, 0) == lax.broadcasted_iota(jnp.int32, tile, 1)
    bias = jnp.where(eye, 1.25, 0.0)
    for start, stop in panels(width):
        grads[1, :, start:stop] = grads[0, start:stop, :].T
    stat_in.wait()

    def gram_step(s, carry):
        total = jnp.zeros((8, PANEL), jnp.float32)
        for start, stop in panels(width):
            gram = scale * dot_f32(grads[s, :stop, :], grads[1 - s, :, start:stop])
            upper = 0.9 * stat_old[s, :stop, start:stop] + gram
            stat[s, :stop, start:stop] = upper
            total = total + lane_sums(upper * upper)
            for low in range(0, start, PANEL):
                high = low + PANEL
                lower = 0.9 * stat_old[s, start:stop, low:high] + gram[low:high].T
                stat[s, start:stop, low:high] = lower
                total = total + lane_sums(lower * lower)
        sums[s] = total
        return carry

    lax.fori_loop(0, 2, gram_step, 0)
    stat_done = pltpu.make_async_copy(stat, stat_out.at[pl.ds(2 * block, 2)], sem_o)
    stat_done.start()

    def root_step(s, carry):
        left_root[...] = root[...]
        z = 2.5 / jnp.sqrt(jnp.sum(sums[s], keepdims=True) + 1e-06)
        root0 = jnp.sqrt(jnp.sqrt(z)).astype(jnp.bfloat16).astype(jnp.float32)
        for start, stop in panels(width):
            for low, high in panels(width):
                scaled = z * stat[s, low:high, start:stop]
                first = -0.25 * scaled
                if low == start:
                    first = bias + first
                first = first.astype(jnp.bfloat16)
                matrix[low:high, start:stop] = scaled.astype(jnp.bfloat16)
                factor[low:high, start:stop] = first
                root[low:high, start:stop] = (root0 * first.astype(jnp.float32)).astype(jnp.bfloat16)

        def next_factor(value, start, stop):
            factor[start:stop, start:stop] = (bias - 0.25 * value[start:]).astype(jnp.bfloat16)
            if start:
                off = (-0.25 * value[:start]).astype(jnp.bfloat16)
                factor[:start, start:stop] = off
                factor[start:stop, :start] = off.T

        def newton(it, inner):
            mirrored(factor, factor, square)
            mirrored(square, square, fourth)
            mirrored(fourth, matrix, matrix, next_factor)
            mirrored(factor, root, root)
            return inner

        lax.fori_loop(0, ITERS - 1, newton, 0)
        return carry

    lax.fori_loop(0, 2, root_step, 0)
    for start, stop in panels(width):
        square[:, start:stop] = dot_f32(left_root[...], grads[0, :, start:stop]).astype(jnp.bfloat16)
    total = jnp.zeros((8, PANEL), jnp.float32)
    for start, stop in panels(width):
        value = dot_f32(square[...], root[:, start:stop])
        fourth[:, start:stop] = value.astype(jnp.bfloat16)
        total = total + lane_sums(value * value)
    if whole:
        sends = [pltpu.make_async_copy(fourth, prod_outs[0], sem_p.at[0])]
    else:
        sends = [
            pltpu.make_async_copy(fourth.at[rows_of(partner), :], prod_outs[n], sem_p.at[n])
            for n, partner in enumerate((0, *partners))
        ]
    for send in sends:
        send.start()
    squares_out[...] = jnp.broadcast_to(jnp.sum(total, keepdims=True), squares_out.shape)
    stat_done.wait()
    for send in sends:
        send.wait()


def block_call(block, partners, whole, me, scale, own, received, statistics, carried):
    dev_rows, width = own.shape[2:]
    square = (width, width)
    hbm = pl.BlockSpec(memory_space=pltpu.HBM)
    smem = pl.BlockSpec(memory_space=pltpu.SMEM)
    operands = [me, scale, own, statistics, *received]
    in_specs = [smem, smem] + [hbm] * (2 + len(received))
    aliases = {}
    if carried is not None:
        aliases = {len(operands): 0}
        operands.append(carried)
        in_specs.append(hbm)
    pieces = 1 if whole else len(partners) + 1
    piece_shape = square if whole else (dev_rows, width)
    flops = 2 * width ** 3 * 16
    results = pl.pallas_call(
        functools.partial(block_kernel, block, partners, whole),
        out_shape=(
            jax.ShapeDtypeStruct(statistics.shape, jnp.float32),
            *[jax.ShapeDtypeStruct(piece_shape, jnp.bfloat16) for _ in range(pieces)],
            jax.ShapeDtypeStruct((1, 128), jnp.float32),
        ),
        in_specs=in_specs,
        out_specs=(hbm, *[hbm] * pieces, pl.BlockSpec(memory_space=pltpu.VMEM)),
        scratch_shapes=[
            pltpu.VMEM((2,) + square, jnp.bfloat16),
            pltpu.VMEM((2,) + square, jnp.float32),
            pltpu.VMEM((2,) + square, jnp.float32),
            *[pltpu.VMEM(square, jnp.bfloat16) for _ in range(6)],
            pltpu.VMEM((2, 8, PANEL), jnp.float32),
            pltpu.SemaphoreType.DMA((len(partners) + 1,)),
            pltpu.SemaphoreType.DMA,
            pltpu.SemaphoreType.DMA,
            pltpu.SemaphoreType.DMA((len(partners) + 1,)),
        ],
        input_output_aliases=aliases,
        compiler_params=pltpu.CompilerParams(vmem_limit_bytes=58 * 1024 * 1024),
        cost_estimate=pl.CostEstimate(flops=flops, bytes_accessed=20 * width * width, transcendentals=0),
    )(*operands)
    return results[0], results[1:-1], results[-1]


def scale_rows(ratio_ref, rows_ref, *rest):
    out_ref = rest[-1]
    out_ref[...] = ratio_ref[0] * rows_ref[...].astype(jnp.float32)


def scale_whole(chunk, chunks, ratio, rows, carried):
    owners, dev_rows, width = rows.shape
    step = max(1, owners // 4)
    operands = [ratio, rows]
    in_specs = [
        pl.BlockSpec(memory_space=pltpu.SMEM),
        pl.BlockSpec((step, dev_rows, width), lambda i: (i, 0, 0)),
    ]
    aliases = {}
    if carried is not None:
        aliases = {len(operands): 0}
        operands.append(carried)
        in_specs.append(pl.BlockSpec(memory_space=pltpu.HBM))
    return pl.pallas_call(
        scale_rows,
        grid=(owners // step,),
        out_shape=jax.ShapeDtypeStruct((owners, chunks, dev_rows, width), jnp.float32),
        in_specs=in_specs,
        out_specs=pl.BlockSpec((step, None, dev_rows, width), lambda i: (i, chunk, 0, 0)),
        input_output_aliases=aliases,
        compiler_params=pltpu.CompilerParams(vmem_limit_bytes=16 * 1024 * 1024),
        cost_estimate=pl.CostEstimate(flops=rows.size, bytes_accessed=6 * rows.size, transcendentals=0),
    )(*operands)


def scale_kernel(chunk, partners, me_ref, ratio_ref, *rest):
    count = len(partners) + 1
    pieces = rest[:count]
    out_ref, narrow, wide, sem_in, sem_out = rest[-5:]
    me = me_ref[0]
    loads = [pltpu.make_async_copy(pieces[n], narrow.at[n], sem_in.at[n]) for n in range(count)]
    for load in loads:
        load.start()
    stores = []
    for n, partner in enumerate((0, *partners)):
        loads[n].wait()
        wide[n] = ratio_ref[0] * narrow[n].astype(jnp.float32)
        store = pltpu.make_async_copy(wide.at[n], out_ref.at[me ^ partner, chunk], sem_out.at[n])
        store.start()
        stores.append(store)
    for store in stores:
        store.wait()


def scale_pieces(chunk, chunks, partners, me, ratio, pieces, carried):
    dev_rows, width = pieces[0].shape
    owners = len(pieces)
    hbm = pl.BlockSpec(memory_space=pltpu.HBM)
    smem = pl.BlockSpec(memory_space=pltpu.SMEM)
    operands = [me, ratio, *pieces]
    in_specs = [smem, smem] + [hbm] * owners
    aliases = {}
    if carried is not None:
        aliases = {len(operands): 0}
        operands.append(carried)
        in_specs.append(hbm)
    size = owners * dev_rows * width
    return pl.pallas_call(
        functools.partial(scale_kernel, chunk, partners),
        out_shape=jax.ShapeDtypeStruct((owners, chunks, dev_rows, width), jnp.float32),
        in_specs=in_specs,
        out_specs=hbm,
        scratch_shapes=[
            pltpu.VMEM((owners, dev_rows, width), jnp.bfloat16),
            pltpu.VMEM((owners, dev_rows, width), jnp.float32),
            pltpu.SemaphoreType.DMA((owners,)),
            pltpu.SemaphoreType.DMA((owners,)),
        ],
        input_output_aliases=aliases,
        compiler_params=pltpu.CompilerParams(vmem_limit_bytes=16 * 1024 * 1024),
        cost_estimate=pl.CostEstimate(flops=size, bytes_accessed=6 * size, transcendentals=0),
    )(*operands)


def partner_order(owners):
    half = owners // 2
    order = (owners - 2, *range(2, half), owners - 1, *range(half, owners - 2), 1)
    return tuple(dict.fromkeys(d for d in order if 0 < d < owners))


def swap(piece, partner):
    size = lax.axis_size("dp")
    return lax.ppermute(piece, "dp", [(i, i ^ partner) for i in range(size)])


def sum_over(value, axis):
    size = lax.axis_size(axis)
    parts = [
        lax.ppermute(value, axis, [(i, (i + shift) % size) for i in range(size)])
        for shift in range(1, size)
    ]
    for part in parts:
        value = value + part
    return value


def exchange(pieces):
    return lax.all_to_all(pieces, "dp", split_axis=0, concat_axis=0, tiled=True)


def on_device(gradients, statistics, accumulator):
    owners = lax.axis_size("dp")
    row_blocks, col_blocks, dev_rows, block_width = gradients.shape
    blocks = row_blocks * col_blocks
    chunks = statistics.shape[1] // 2
    by_owner = gradients.reshape(owners, chunks, dev_rows, block_width)
    grads_wide = gradients.astype(jnp.float32)
    squares = jnp.full((1, 128), jnp.sum(grads_wide * grads_wide))
    partners = partner_order(owners)
    own_index = lax.axis_index("dp")
    me = own_index.astype(jnp.int32).reshape(1)
    received = []
    source = by_owner
    for c in range(chunks):
        parts = []
        for partner in partners:
            piece = lax.dynamic_slice(
                source, (own_index ^ partner, c, 0, 0), (1, 1, dev_rows, block_width)
            )
            source, piece = lax.optimization_barrier((source, piece))
            parts.append(swap(piece.reshape(dev_rows, block_width), partner))
        received.append(parts)
    grad_total = sum_over(squares, "mp")
    grad_total = sum_over(grad_total, "dp")[0, 0]
    entries = blocks * dev_rows * block_width * owners * lax.axis_size("mp")
    clip_factor = jnp.minimum(1.0, jnp.sqrt(entries / (grad_total + 1e-06)))
    scale = (0.1 / block_width * clip_factor * clip_factor).reshape(1)
    scaled = clip_factor * grads_wide
    accumulated = accumulator + scaled * scaled
    graft_step = scaled / jnp.sqrt(accumulated)
    graft_squares = jnp.sum(graft_step * graft_step)
    statistics_new = None
    returned = []
    update_squares = jnp.zeros((1, 128), jnp.float32)
    for c in range(chunks):
        whole = c + 1 < chunks
        statistics_new, product, part = block_call(
            c, partners, whole, me, scale, by_owner, received[c], statistics[0], statistics_new
        )
        update_squares = update_squares + part
        if whole:
            returned.append(exchange(product[0].reshape(owners, dev_rows, block_width)))
        else:
            parts = [product[0]]
            for n, partner in enumerate(partners):
                parts.append(swap(product[n + 1], partner))
            returned.append(parts)
    lanes = lax.broadcasted_iota(jnp.int32, (1, 128), 1)
    sums = jnp.where(lanes == 0, graft_squares, update_squares)
    sums = sum_over(sums, "mp")
    sums = sum_over(sums, "dp")
    graft_ratio = jnp.sqrt(sums[0, :1] / (sums[0, 1:2] + 1e-06))
    update = None
    for c in range(chunks):
        if c + 1 < chunks:
            update = scale_whole(c, chunks, graft_ratio, returned[c], update)
        else:
            update = scale_pieces(c, chunks, partners, me, graft_ratio, returned[c], update)
    return (update.reshape(gradients.shape), statistics_new[None], accumulated)


def solution(mesh):
    def run(gradients, statistics, accumulator):
        if statistics.shape[1] != 4:
            return on_device_plain(gradients, statistics, accumulator)
        return on_device(gradients, statistics, accumulator)

    return jax.shard_map(
        run,
        mesh=mesh,
        in_specs=(P(None, "mp", "dp", None), P("mp", "dp", None, None), P(None, "mp", "dp", None)),
        out_specs=(P(None, "mp", "dp", None), P("mp", "dp", None, None), P(None, "mp", "dp", None)),
        check_vma=False,
    )
```

```python
import functools

import jax
import jax.numpy as jnp
from jax import lax
from jax.experimental import pallas as pl
from jax.experimental.pallas import tpu as pltpu
from jax.sharding import PartitionSpec as P


ITERS = 3
PANEL = 256


def partner_2(value, axis, distance):
    return lax.ppermute(value, axis, [(i, i ^ 1 << distance) for i in range(lax.axis_size(axis))])


def batch_dot(left, right):
    return jnp.einsum("kij,kjl->kil", left, right, preferred_element_type=jnp.float32)


def inverse_roots(statistic):
    block_width = statistic.shape[-1]
    identity = jnp.eye(block_width, dtype=jnp.float32)
    frob_norms = jnp.sqrt(jnp.sum(statistic * statistic, axis=(1, 2)) + 1e-06)
    newton_scale = (2.5 / frob_norms)[:, None, None]
    matrix = newton_scale * statistic
    root_iter = jnp.sqrt(jnp.sqrt(newton_scale)) * identity
    for iteration in range(ITERS):
        factor = (1.25 * identity - 0.25 * matrix).astype(jnp.bfloat16)
        root_iter = batch_dot(root_iter.astype(jnp.bfloat16), factor)
        if iteration + 1 < ITERS:
            square = batch_dot(factor, factor).astype(jnp.bfloat16)
            fourth = batch_dot(square, square).astype(jnp.bfloat16)
            matrix = batch_dot(fourth, matrix.astype(jnp.bfloat16))
    return root_iter


def on_device_plain(gradients, statistics, accumulator):
    owners = lax.axis_size("dp")
    own_index = lax.axis_index("dp")
    row_blocks, col_blocks, dev_rows, block_width = gradients.shape
    blocks = row_blocks * col_blocks
    owned_factors = statistics.shape[1]
    split_pairs = owned_factors == 1
    half_rows = dev_rows // 2
    parity = own_index % 2
    left_side = parity == 0
    by_block = gradients.reshape(blocks, dev_rows, block_width)
    grads_wide = gradients.astype(jnp.float32)
    grad_total = lax.psum(jnp.sum(grads_wide * grads_wide), ("dp", "mp"))
    entries = blocks * dev_rows * block_width * owners * lax.axis_size("mp")
    clip_factor = jnp.minimum(1.0, jnp.sqrt(entries / (grad_total + 1e-06)))
    scaled = clip_factor * grads_wide
    accumulated = accumulator + scaled * scaled
    graft_step = scaled / jnp.sqrt(accumulated)
    graft_squares = jnp.sum(graft_step * graft_step)
    row_parts = 2 if split_pairs else 1
    row_units = by_block.reshape(blocks * row_parts, dev_rows // row_parts, block_width)
    received = lax.all_to_all(row_units, "dp", split_axis=0, concat_axis=1, tiled=True)
    if split_pairs:
        partner_part = partner_2(received, "dp", 0)
        own_part = received.reshape(owners, 1, half_rows, block_width)
        partner_part = partner_part.reshape(owners, 1, half_rows, block_width)
        ordered = jnp.where(
            left_side,
            jnp.concatenate([own_part, partner_part], 1),
            jnp.concatenate([partner_part, own_part], 1),
        )
        whole_blocks = ordered.reshape(1, owners * dev_rows, block_width)
    else:
        whole_blocks = received
    transposed = jnp.swapaxes(whole_blocks, 1, 2)
    if split_pairs:
        factor_inputs = jnp.where(left_side, whole_blocks, transposed)
    else:
        factor_inputs = jnp.stack([whole_blocks, transposed], 1).reshape(
            owned_factors, block_width, block_width
        )
    gram_matrix = jnp.einsum(
        "kij,klj->kil", factor_inputs, factor_inputs, preferred_element_type=jnp.float32
    )
    statistics_new = (
        0.9 * statistics[0] + 0.1 / block_width * clip_factor * clip_factor * gram_matrix
    )
    root_values = inverse_roots(statistics_new).astype(jnp.bfloat16)
    if split_pairs:
        partner = partner_2(root_values, "dp", 0)
        left_root = jnp.where(left_side, root_values, partner)[0]
        right_root = jnp.where(left_side, partner, root_values)[0]
        left_rows = lax.dynamic_slice_in_dim(
            left_root.reshape(owners, 2, half_rows, block_width), parity, 1, 1
        )
        left_rows = left_rows.reshape(owners * half_rows, block_width)
        left_applied = jnp.dot(
            left_rows, whole_blocks[0], preferred_element_type=jnp.float32
        ).astype(jnp.bfloat16)
        product = jnp.dot(left_applied, right_root, preferred_element_type=jnp.float32)
        pieces = product.reshape(1, owners, half_rows, block_width)
    else:
        root_pairs = root_values.reshape(-1, 2, block_width, block_width)
        left_applied = batch_dot(root_pairs[:, 0], whole_blocks).astype(jnp.bfloat16)
        product = batch_dot(left_applied, root_pairs[:, 1])
        pieces = product.reshape(-1, owners, dev_rows, block_width)
    returned = lax.all_to_all(
        pieces.astype(jnp.bfloat16), "dp", split_axis=1, concat_axis=0, tiled=True
    ).astype(pieces.dtype)
    returned = returned.reshape(row_blocks, col_blocks, dev_rows, block_width)
    graft_total, update_total = lax.psum(
        (graft_squares, jnp.sum(returned * returned)), ("dp", "mp")
    )
    graft_ratio = jnp.sqrt(graft_total / (update_total + 1e-06))
    return (graft_ratio * returned, statistics_new[None], accumulated)


def dot_f32(left, right):
    return jnp.dot(left, right, preferred_element_type=jnp.float32)


def panels(width):
    return [(start, start + PANEL) for start in range(0, width, PANEL)]


def lane_sums(value):
    return jnp.sum(value.reshape(-1, 8, value.shape[-1]), axis=0)


def mirrored(left, right, out, post=None):
    for start, stop in panels(left.shape[0]):
        value = dot_f32(left[:stop, :], right[:, start:stop])
        upper = value.astype(jnp.bfloat16)
        out[:stop, start:stop] = upper
        if start:
            out[start:stop, :start] = upper[:start].T
        if post is not None:
            post(value, start, stop)


def block_kernel(block, partners, whole, me_ref, scale_ref, own_hbm, stat_hbm, *rest):
    received = rest[: len(partners)]
    outs = rest[len(rest) - 17 - (0 if whole else len(partners)):]
    stat_out = outs[0]
    prod_outs = outs[1 : len(outs) - 15]
    (squares_out,
     grads, stat_old, stat, matrix, factor, root, square, fourth, left_root, sums,
     sem_g, sem_s, sem_o, sem_p) = outs[len(outs) - 15:]
    width = grads.shape[1]
    dev_rows = own_hbm.shape[2]
    me = me_ref[0]

    def rows_of(partner):
        return pl.ds(pl.multiple_of((me ^ partner) * dev_rows, dev_rows), dev_rows)

    grad_in = [pltpu.make_async_copy(own_hbm.at[me, block], grads.at[0, rows_of(0), :], sem_g.at[0])]
    for n, partner in enumerate(partners):
        grad_in.append(pltpu.make_async_copy(received[n], grads.at[0, rows_of(partner), :], sem_g.at[n + 1]))
    for copy in grad_in:
        copy.start()

    def stat_load(s):
        return pltpu.make_async_copy(stat_hbm.at[2 * block + s], stat_old.at[s], sem_s.at[s])

    for s in range(2):
        stat_load(s).start()
    for copy in grad_in:
        copy.wait()
    scale = scale_ref[0]
    tile = (PANEL, PANEL)
    eye = lax.broadcasted_iota(jnp.int32, tile, 0) == lax.broadcasted_iota(jnp.int32, tile, 1)
    bias = jnp.where(eye, 1.25, 0.0)
    for start, stop in panels(width):
        grads[1, :, start:stop] = grads[0, start:stop, :].T

    def gram_step(s, carry):
        stat_load(s).wait()
        total = jnp.zeros((8, PANEL), jnp.float32)
        for start, stop in panels(width):
            gram = scale * dot_f32(grads[s, :stop, :], grads[1 - s, :, start:stop])
            upper = 0.9 * stat_old[s, :stop, start:stop] + gram
            stat[s, :stop, start:stop] = upper
            total = total + lane_sums(upper * upper)
            for low in range(0, start, PANEL):
                high = low + PANEL
                lower = 0.9 * stat_old[s, start:stop, low:high] + gram[low:high].T
                stat[s, start:stop, low:high] = lower
                total = total + lane_sums(lower * lower)
        sums[s] = total
        return carry

    lax.fori_loop(0, 2, gram_step, 0)
    stat_done = pltpu.make_async_copy(stat, stat_out.at[pl.ds(2 * block, 2)], sem_o)
    stat_done.start()

    def root_step(s, carry):
        z = 2.5 / jnp.sqrt(jnp.sum(sums[s], keepdims=True) + 1e-06)
        root0 = jnp.sqrt(jnp.sqrt(z)).astype(jnp.bfloat16)

        def begin(row, cols, offset):
            scaled = z * stat[s, row, cols]
            first = (offset - 0.25 * scaled).astype(jnp.bfloat16)
            matrix[row, cols] = scaled.astype(jnp.bfloat16)
            factor[row, cols] = first
            root[row, cols] = root0 * first

        def begin_panel(n, inner):
            row = pl.ds(pl.multiple_of(n * PANEL, PANEL), PANEL)
            for start, stop in panels(width):
                begin(row, slice(start, stop), 0.0)
            begin(row, row, bias)
            return inner

        lax.fori_loop(0, width // PANEL, begin_panel, 0)

        def next_factor(value, start, stop):
            factor[start:stop, start:stop] = (bias - 0.25 * value[start:]).astype(jnp.bfloat16)
            if start:
                off = (-0.25 * value[:start]).astype(jnp.bfloat16)
                factor[:start, start:stop] = off
                factor[start:stop, :start] = off.T

        def newton(it, inner):
            mirrored(factor, factor, square)
            mirrored(square, square, fourth)
            mirrored(fourth, matrix, matrix, next_factor)
            mirrored(factor, root, root)
            return inner

        lax.fori_loop(0, ITERS - 1, newton, 0)

        @pl.when(s == 0)
        def _():
            left_root[...] = root[...]

        return carry

    lax.fori_loop(0, 2, root_step, 0)
    for start, stop in panels(width):
        square[:, start:stop] = dot_f32(left_root[...], grads[0, :, start:stop]).astype(jnp.bfloat16)
    total = jnp.zeros((8, PANEL), jnp.float32)
    for start, stop in panels(width):
        value = dot_f32(square[...], root[:, start:stop])
        fourth[:, start:stop] = value.astype(jnp.bfloat16)
        total = total + lane_sums(value * value)
    if whole:
        sends = [pltpu.make_async_copy(fourth, prod_outs[0], sem_p.at[0])]
    else:
        sends = [
            pltpu.make_async_copy(fourth.at[rows_of(partner), :], prod_outs[n], sem_p.at[n])
            for n, partner in enumerate((0, *partners))
        ]
    for send in sends:
        send.start()
    squares_out[...] = jnp.broadcast_to(jnp.sum(total, keepdims=True), squares_out.shape)
    stat_done.wait()
    for send in sends:
        send.wait()


def block_call(block, partners, whole, me, scale, own, received, statistics, carried):
    dev_rows, width = own.shape[2:]
    square = (width, width)
    hbm = pl.BlockSpec(memory_space=pltpu.HBM)
    smem = pl.BlockSpec(memory_space=pltpu.SMEM)
    operands = [me, scale, own, statistics, *received]
    in_specs = [smem, smem] + [hbm] * (2 + len(received))
    aliases = {}
    if carried is not None:
        aliases = {len(operands): 0}
        operands.append(carried)
        in_specs.append(hbm)
    pieces = 1 if whole else len(partners) + 1
    piece_shape = square if whole else (dev_rows, width)
    flops = 2 * width ** 3 * 16
    results = pl.pallas_call(
        functools.partial(block_kernel, block, partners, whole),
        out_shape=(
            jax.ShapeDtypeStruct(statistics.shape, jnp.float32),
            *[jax.ShapeDtypeStruct(piece_shape, jnp.bfloat16) for _ in range(pieces)],
            jax.ShapeDtypeStruct((1, 128), jnp.float32),
        ),
        in_specs=in_specs,
        out_specs=(hbm, *[hbm] * pieces, pl.BlockSpec(memory_space=pltpu.VMEM)),
        scratch_shapes=[
            pltpu.VMEM((2,) + square, jnp.bfloat16),
            pltpu.VMEM((2,) + square, jnp.float32),
            pltpu.VMEM((2,) + square, jnp.float32),
            *[pltpu.VMEM(square, jnp.bfloat16) for _ in range(6)],
            pltpu.VMEM((2, 8, PANEL), jnp.float32),
            pltpu.SemaphoreType.DMA((len(partners) + 1,)),
            pltpu.SemaphoreType.DMA((2,)),
            pltpu.SemaphoreType.DMA,
            pltpu.SemaphoreType.DMA((len(partners) + 1,)),
        ],
        input_output_aliases=aliases,
        compiler_params=pltpu.CompilerParams(vmem_limit_bytes=58 * 1024 * 1024),
        cost_estimate=pl.CostEstimate(flops=flops, bytes_accessed=20 * width * width, transcendentals=0),
    )(*operands)
    return results[0], results[1:-1], results[-1]


def gather_kernel(chunk, partners, me_ref, grad_hbm, *rest):
    count = len(partners)
    outs = rest[:count]
    squares_out, held, sem_in, sem_out = rest[count:]
    me = me_ref[0]
    loads = [
        pltpu.make_async_copy(grad_hbm.at[me ^ partner, chunk], held.at[n], sem_in.at[n])
        for n, partner in enumerate((*partners, 0))
    ]
    for load in loads:
        load.start()
    stores = []
    for n in range(count):
        loads[n].wait()
        store = pltpu.make_async_copy(held.at[n], outs[n], sem_out.at[n])
        store.start()
        stores.append(store)
    loads[count].wait()
    rows = 16

    def add_rows(i, total):
        at = pl.multiple_of(i * rows, rows)
        for n in range(count + 1):
            wide = held[n, pl.ds(at, rows), :].astype(jnp.float32)
            total = total + wide * wide
        return total

    width = held.shape[2]
    total = lax.fori_loop(0, held.shape[1] // rows, add_rows, jnp.zeros((rows, width), jnp.float32))
    squares_out[...] = jnp.broadcast_to(jnp.sum(total, keepdims=True), squares_out.shape)
    for store in stores:
        store.wait()


def gather_call(chunk, partners, me, by_owner):
    dev_rows, width = by_owner.shape[2:]
    hbm = pl.BlockSpec(memory_space=pltpu.HBM)
    count = len(partners)
    size = (count + 1) * dev_rows * width
    results = pl.pallas_call(
        functools.partial(gather_kernel, chunk, partners),
        out_shape=(
            *[jax.ShapeDtypeStruct((dev_rows, width), jnp.bfloat16) for _ in partners],
            jax.ShapeDtypeStruct((1, 128), jnp.float32),
        ),
        in_specs=[pl.BlockSpec(memory_space=pltpu.SMEM), hbm],
        out_specs=(*[hbm] * count, pl.BlockSpec(memory_space=pltpu.VMEM)),
        scratch_shapes=[
            pltpu.VMEM((count + 1, dev_rows, width), jnp.bfloat16),
            pltpu.SemaphoreType.DMA((count + 1,)),
            pltpu.SemaphoreType.DMA((count,)),
        ],
        compiler_params=pltpu.CompilerParams(vmem_limit_bytes=16 * 1024 * 1024),
        cost_estimate=pl.CostEstimate(flops=2 * size, bytes_accessed=4 * size, transcendentals=0),
    )(me, by_owner)
    return results[:-1], results[-1]


def scale_kernel(chunk, targets, me_ref, ratio_ref, *rest):
    pieces = rest[: len(targets)]
    out_ref, narrow, wide, sem_in, sem_out = rest[-5:]
    me = me_ref[0]
    if len(rest) < len(targets) + 5:
        pieces = [rest[0].at[n] for n in range(len(targets))]
    loads = [pltpu.make_async_copy(piece, narrow.at[n], sem_in.at[n]) for n, piece in enumerate(pieces)]
    for load in loads:
        load.start()
    stores = []
    for n, target in enumerate(targets):
        loads[n].wait()
        wide[n] = ratio_ref[0] * narrow[n].astype(jnp.float32)
        owner = n if target is None else me ^ target
        store = pltpu.make_async_copy(wide.at[n], out_ref.at[owner, chunk], sem_out.at[n])
        store.start()
        stores.append(store)
    for store in stores:
        store.wait()


def scale_call(chunk, out_shape, targets, me, ratio, pieces, carried):
    dev_rows, width = out_shape[2:]
    count = len(targets)
    hbm = pl.BlockSpec(memory_space=pltpu.HBM)
    smem = pl.BlockSpec(memory_space=pltpu.SMEM)
    operands = [me, ratio, *pieces]
    in_specs = [smem, smem] + [hbm] * len(pieces)
    aliases = {}
    if carried is not None:
        aliases = {len(operands): 0}
        operands.append(carried)
        in_specs.append(hbm)
    size = count * dev_rows * width
    return pl.pallas_call(
        functools.partial(scale_kernel, chunk, targets),
        out_shape=jax.ShapeDtypeStruct(out_shape, jnp.float32),
        in_specs=in_specs,
        out_specs=hbm,
        scratch_shapes=[
            pltpu.VMEM((count, dev_rows, width), jnp.bfloat16),
            pltpu.VMEM((count, dev_rows, width), jnp.float32),
            pltpu.SemaphoreType.DMA((count,)),
            pltpu.SemaphoreType.DMA((count,)),
        ],
        input_output_aliases=aliases,
        compiler_params=pltpu.CompilerParams(vmem_limit_bytes=16 * 1024 * 1024),
        cost_estimate=pl.CostEstimate(flops=size, bytes_accessed=6 * size, transcendentals=0),
    )(*operands)


def partner_order(owners):
    half = owners // 2
    order = (owners - 2, owners - 1, *range(2, half), *range(half, owners - 2), 1)
    return tuple(dict.fromkeys(d for d in order if 0 < d < owners))


def swap(piece, partner):
    size = lax.axis_size("dp")
    return lax.ppermute(piece, "dp", [(i, i ^ partner) for i in range(size)])


def sum_over(value, axis):
    size = lax.axis_size(axis)
    parts = [
        lax.ppermute(value, axis, [(i, (i + shift) % size) for i in range(size)])
        for shift in range(1, size)
    ]
    for part in parts:
        value = value + part
    return value


def exchange(pieces):
    return lax.all_to_all(pieces, "dp", split_axis=0, concat_axis=0, tiled=True)


def on_device(gradients, statistics, accumulator):
    owners = lax.axis_size("dp")
    row_blocks, col_blocks, dev_rows, block_width = gradients.shape
    blocks = row_blocks * col_blocks
    chunks = statistics.shape[1] // 2
    by_owner = gradients.reshape(owners, chunks, dev_rows, block_width)
    grads_wide = gradients.astype(jnp.float32)
    partners = partner_order(owners)
    me = lax.axis_index("dp").astype(jnp.int32).reshape(1)
    squares = jnp.zeros((1, 128), jnp.float32)
    received = []
    for c in range(chunks):
        pieces, part = gather_call(c, partners, me, by_owner)
        squares = squares + part
        parts = []
        for partner, piece in zip(partners, pieces):
            parts.append(swap(piece, partner))
        received.append(parts)
    grad_total = sum_over(squares, "mp")
    grad_total = sum_over(grad_total, "dp")[0, 0]
    entries = blocks * dev_rows * block_width * owners * lax.axis_size("mp")
    clip_factor = jnp.minimum(1.0, jnp.sqrt(entries / (grad_total + 1e-06)))
    scale = (0.1 / block_width * clip_factor * clip_factor).reshape(1)
    scaled = clip_factor * grads_wide
    accumulated = accumulator + scaled * scaled
    graft_step = scaled / jnp.sqrt(accumulated)
    graft_squares = jnp.sum(graft_step * graft_step)
    statistics_new = None
    returned = []
    update_squares = jnp.zeros((1, 128), jnp.float32)
    for c in range(chunks):
        whole = c + 1 < chunks
        statistics_new, product, part = block_call(
            c, partners, whole, me, scale, by_owner, received[c], statistics[0], statistics_new
        )
        update_squares = update_squares + part
        if whole:
            returned.append([exchange(product[0].reshape(owners, dev_rows, block_width))])
        else:
            parts = [product[0]]
            for n, partner in enumerate(partners):
                parts.append(swap(product[n + 1], partner))
            returned.append(parts)
    lanes = lax.broadcasted_iota(jnp.int32, (1, 128), 1)
    sums = jnp.where(lanes == 0, graft_squares, update_squares)
    sums = sum_over(sums, "mp")
    sums = sum_over(sums, "dp")
    graft_ratio = jnp.sqrt(sums[0, :1] / (sums[0, 1:2] + 1e-06))
    update = None
    out_shape = (owners, chunks, dev_rows, block_width)
    for c in range(chunks - 1):
        update = scale_call(c, out_shape, (None,) * owners, me, graft_ratio, returned[c], update)
    late = partners[-2]
    groups = (tuple(d for d in (0, *partners) if d != late), (late,))
    for group in groups:
        pieces = [dict(zip((0, *partners), returned[-1]))[d] for d in group]
        update = scale_call(chunks - 1, out_shape, group, me, graft_ratio, pieces, update)
    return (update.reshape(gradients.shape), statistics_new[None], accumulated)


def solution(mesh):
    def run(gradients, statistics, accumulator):
        if statistics.shape[1] != 4:
            return on_device_plain(gradients, statistics, accumulator)
        return on_device(gradients, statistics, accumulator)

    return jax.shard_map(
        run,
        mesh=mesh,
        in_specs=(P(None, "mp", "dp", None), P("mp", "dp", None, None), P(None, "mp", "dp", None)),
        out_specs=(P(None, "mp", "dp", None), P("mp", "dp", None, None), P(None, "mp", "dp", None)),
        check_vma=False,
    )
```

```python
import functools

import jax
import jax.numpy as jnp
from jax import lax
from jax.experimental import pallas as pl
from jax.experimental.pallas import tpu as pltpu
from jax.sharding import PartitionSpec as P


ITERS = 3
PANEL = 256


def partner_2(value, axis, distance):
    return lax.ppermute(value, axis, [(i, i ^ 1 << distance) for i in range(lax.axis_size(axis))])


def batch_dot(left, right):
    return jnp.einsum("kij,kjl->kil", left, right, preferred_element_type=jnp.float32)


def inverse_roots(statistic):
    block_width = statistic.shape[-1]
    identity = jnp.eye(block_width, dtype=jnp.float32)
    frob_norms = jnp.sqrt(jnp.sum(statistic * statistic, axis=(1, 2)) + 1e-06)
    newton_scale = (2.5 / frob_norms)[:, None, None]
    matrix = newton_scale * statistic
    root_iter = jnp.sqrt(jnp.sqrt(newton_scale)) * identity
    for iteration in range(ITERS):
        factor = (1.25 * identity - 0.25 * matrix).astype(jnp.bfloat16)
        root_iter = batch_dot(root_iter.astype(jnp.bfloat16), factor)
        if iteration + 1 < ITERS:
            square = batch_dot(factor, factor).astype(jnp.bfloat16)
            fourth = batch_dot(square, square).astype(jnp.bfloat16)
            matrix = batch_dot(fourth, matrix.astype(jnp.bfloat16))
    return root_iter


def on_device_plain(gradients, statistics, accumulator):
    owners = lax.axis_size("dp")
    own_index = lax.axis_index("dp")
    row_blocks, col_blocks, dev_rows, block_width = gradients.shape
    blocks = row_blocks * col_blocks
    owned_factors = statistics.shape[1]
    split_pairs = owned_factors == 1
    half_rows = dev_rows // 2
    parity = own_index % 2
    left_side = parity == 0
    by_block = gradients.reshape(blocks, dev_rows, block_width)
    grads_wide = gradients.astype(jnp.float32)
    grad_total = lax.psum(jnp.sum(grads_wide * grads_wide), ("dp", "mp"))
    entries = blocks * dev_rows * block_width * owners * lax.axis_size("mp")
    clip_factor = jnp.minimum(1.0, jnp.sqrt(entries / (grad_total + 1e-06)))
    scaled = clip_factor * grads_wide
    accumulated = accumulator + scaled * scaled
    graft_step = scaled / jnp.sqrt(accumulated)
    graft_squares = jnp.sum(graft_step * graft_step)
    row_parts = 2 if split_pairs else 1
    row_units = by_block.reshape(blocks * row_parts, dev_rows // row_parts, block_width)
    received = lax.all_to_all(row_units, "dp", split_axis=0, concat_axis=1, tiled=True)
    if split_pairs:
        partner_part = partner_2(received, "dp", 0)
        own_part = received.reshape(owners, 1, half_rows, block_width)
        partner_part = partner_part.reshape(owners, 1, half_rows, block_width)
        ordered = jnp.where(
            left_side,
            jnp.concatenate([own_part, partner_part], 1),
            jnp.concatenate([partner_part, own_part], 1),
        )
        whole_blocks = ordered.reshape(1, owners * dev_rows, block_width)
    else:
        whole_blocks = received
    transposed = jnp.swapaxes(whole_blocks, 1, 2)
    if split_pairs:
        factor_inputs = jnp.where(left_side, whole_blocks, transposed)
    else:
        factor_inputs = jnp.stack([whole_blocks, transposed], 1).reshape(
            owned_factors, block_width, block_width
        )
    gram_matrix = jnp.einsum(
        "kij,klj->kil", factor_inputs, factor_inputs, preferred_element_type=jnp.float32
    )
    statistics_new = (
        0.9 * statistics[0] + 0.1 / block_width * clip_factor * clip_factor * gram_matrix
    )
    root_values = inverse_roots(statistics_new).astype(jnp.bfloat16)
    if split_pairs:
        partner = partner_2(root_values, "dp", 0)
        left_root = jnp.where(left_side, root_values, partner)[0]
        right_root = jnp.where(left_side, partner, root_values)[0]
        left_rows = lax.dynamic_slice_in_dim(
            left_root.reshape(owners, 2, half_rows, block_width), parity, 1, 1
        )
        left_rows = left_rows.reshape(owners * half_rows, block_width)
        left_applied = jnp.dot(
            left_rows, whole_blocks[0], preferred_element_type=jnp.float32
        ).astype(jnp.bfloat16)
        product = jnp.dot(left_applied, right_root, preferred_element_type=jnp.float32)
        pieces = product.reshape(1, owners, half_rows, block_width)
    else:
        root_pairs = root_values.reshape(-1, 2, block_width, block_width)
        left_applied = batch_dot(root_pairs[:, 0], whole_blocks).astype(jnp.bfloat16)
        product = batch_dot(left_applied, root_pairs[:, 1])
        pieces = product.reshape(-1, owners, dev_rows, block_width)
    returned = lax.all_to_all(
        pieces.astype(jnp.bfloat16), "dp", split_axis=1, concat_axis=0, tiled=True
    ).astype(pieces.dtype)
    returned = returned.reshape(row_blocks, col_blocks, dev_rows, block_width)
    graft_total, update_total = lax.psum(
        (graft_squares, jnp.sum(returned * returned)), ("dp", "mp")
    )
    graft_ratio = jnp.sqrt(graft_total / (update_total + 1e-06))
    return (graft_ratio * returned, statistics_new[None], accumulated)


def dot_f32(left, right):
    return jnp.dot(left, right, preferred_element_type=jnp.float32)


def panels(width):
    return [(start, start + PANEL) for start in range(0, width, PANEL)]


def lane_sums(value):
    return jnp.sum(value.reshape(-1, 8, value.shape[-1]), axis=0)


def mirrored(left, right, out, post=None):
    for start, stop in panels(left.shape[0]):
        value = dot_f32(left[:stop, :], right[:, start:stop])
        upper = value.astype(jnp.bfloat16)
        out[:stop, start:stop] = upper
        if start:
            out[start:stop, :start] = upper[:start].T
        if post is not None:
            post(value, start, stop)


def block_kernel(block, partners, whole, me_ref, scale_ref, own_hbm, stat_hbm, *rest):
    received = rest[: len(partners)]
    outs = rest[len(rest) - 17 - (0 if whole else len(partners)):]
    stat_out = outs[0]
    prod_outs = outs[1 : len(outs) - 15]
    (squares_out,
     grads, stat_old, stat, matrix, factor, root, square, fourth, left_root, sums,
     sem_g, sem_s, sem_o, sem_p) = outs[len(outs) - 15:]
    width = grads.shape[1]
    dev_rows = own_hbm.shape[2]
    me = me_ref[0]

    def rows_of(partner):
        return pl.ds(pl.multiple_of((me ^ partner) * dev_rows, dev_rows), dev_rows)

    grad_in = [pltpu.make_async_copy(own_hbm.at[me, block], grads.at[0, rows_of(0), :], sem_g.at[0])]
    for n, partner in enumerate(partners):
        grad_in.append(pltpu.make_async_copy(received[n], grads.at[0, rows_of(partner), :], sem_g.at[n + 1]))
    for copy in grad_in:
        copy.start()

    def stat_load(s):
        return pltpu.make_async_copy(stat_hbm.at[2 * block + s], stat_old.at[s], sem_s.at[s])

    for s in range(2):
        stat_load(s).start()
    for copy in grad_in:
        copy.wait()
    scale = scale_ref[0]
    tile = (PANEL, PANEL)
    eye = lax.broadcasted_iota(jnp.int32, tile, 0) == lax.broadcasted_iota(jnp.int32, tile, 1)
    bias = jnp.where(eye, 1.25, 0.0)
    for start, stop in panels(width):
        grads[1, :, start:stop] = grads[0, start:stop, :].T

    def gram_step(s, carry):
        stat_load(s).wait()
        total = jnp.zeros((8, PANEL), jnp.float32)
        for start, stop in panels(width):
            gram = scale * dot_f32(grads[s, :stop, :], grads[1 - s, :, start:stop])
            upper = 0.9 * stat_old[s, :stop, start:stop] + gram
            stat[s, :stop, start:stop] = upper
            total = total + lane_sums(upper * upper)
            for low in range(0, start, PANEL):
                high = low + PANEL
                lower = 0.9 * stat_old[s, start:stop, low:high] + gram[low:high].T
                stat[s, start:stop, low:high] = lower
                total = total + lane_sums(lower * lower)
        sums[s] = total
        return carry

    lax.fori_loop(0, 2, gram_step, 0)
    stat_done = pltpu.make_async_copy(stat, stat_out.at[pl.ds(2 * block, 2)], sem_o)
    stat_done.start()

    def root_step(s, carry):
        z = 2.5 / jnp.sqrt(jnp.sum(sums[s], keepdims=True) + 1e-06)
        root0 = jnp.sqrt(jnp.sqrt(z)).astype(jnp.bfloat16)

        def begin(row, cols, offset):
            scaled = z * stat[s, row, cols]
            first = (offset - 0.25 * scaled).astype(jnp.bfloat16)
            matrix[row, cols] = scaled.astype(jnp.bfloat16)
            factor[row, cols] = first
            root[row, cols] = root0 * first

        def begin_panel(n, inner):
            row = pl.ds(pl.multiple_of(n * PANEL, PANEL), PANEL)
            for start, stop in panels(width):
                begin(row, slice(start, stop), 0.0)
            begin(row, row, bias)
            return inner

        lax.fori_loop(0, width // PANEL, begin_panel, 0)

        def next_factor(value, start, stop):
            factor[start:stop, start:stop] = (bias - 0.25 * value[start:]).astype(jnp.bfloat16)
            if start:
                off = (-0.25 * value[:start]).astype(jnp.bfloat16)
                factor[:start, start:stop] = off
                factor[start:stop, :start] = off.T

        def newton(it, inner):
            mirrored(factor, factor, square)
            mirrored(square, square, fourth)
            mirrored(fourth, matrix, matrix, next_factor)
            mirrored(factor, root, root)
            return inner

        lax.fori_loop(0, ITERS - 1, newton, 0)

        @pl.when(s == 0)
        def _():
            left_root[...] = root[...]

        return carry

    lax.fori_loop(0, 2, root_step, 0)
    for start, stop in panels(width):
        square[:, start:stop] = dot_f32(left_root[...], grads[0, :, start:stop]).astype(jnp.bfloat16)
    sends = []
    if whole:
        total = jnp.zeros((8, width), jnp.float32)
        for n, (start, stop) in enumerate(panels(width)):
            value = dot_f32(square[start:stop, :], root[...])
            fourth[start:stop, :] = value.astype(jnp.bfloat16)
            total = total + lane_sums(value * value)
            send = pltpu.make_async_copy(fourth.at[start:stop, :], prod_outs[0].at[start:stop, :], sem_p.at[n])
            send.start()
            sends.append(send)
    else:
        total = jnp.zeros((8, PANEL), jnp.float32)
        for start, stop in panels(width):
            value = dot_f32(square[...], root[:, start:stop])
            fourth[:, start:stop] = value.astype(jnp.bfloat16)
            total = total + lane_sums(value * value)
        for n, partner in enumerate((0, *partners)):
            send = pltpu.make_async_copy(fourth.at[rows_of(partner), :], prod_outs[n], sem_p.at[n])
            send.start()
            sends.append(send)
    squares_out[...] = jnp.broadcast_to(jnp.sum(total, keepdims=True), squares_out.shape)
    stat_done.wait()
    for send in sends:
        send.wait()


def block_call(block, partners, whole, me, scale, own, received, statistics, carried):
    dev_rows, width = own.shape[2:]
    square = (width, width)
    hbm = pl.BlockSpec(memory_space=pltpu.HBM)
    smem = pl.BlockSpec(memory_space=pltpu.SMEM)
    operands = [me, scale, own, statistics, *received]
    in_specs = [smem, smem] + [hbm] * (2 + len(received))
    aliases = {}
    if carried is not None:
        aliases = {len(operands): 0}
        operands.append(carried)
        in_specs.append(hbm)
    pieces = 1 if whole else len(partners) + 1
    piece_shape = square if whole else (dev_rows, width)
    flops = 2 * width ** 3 * 16
    results = pl.pallas_call(
        functools.partial(block_kernel, block, partners, whole),
        out_shape=(
            jax.ShapeDtypeStruct(statistics.shape, jnp.float32),
            *[jax.ShapeDtypeStruct(piece_shape, jnp.bfloat16) for _ in range(pieces)],
            jax.ShapeDtypeStruct((1, 128), jnp.float32),
        ),
        in_specs=in_specs,
        out_specs=(hbm, *[hbm] * pieces, pl.BlockSpec(memory_space=pltpu.VMEM)),
        scratch_shapes=[
            pltpu.VMEM((2,) + square, jnp.bfloat16),
            pltpu.VMEM((2,) + square, jnp.float32),
            pltpu.VMEM((2,) + square, jnp.float32),
            *[pltpu.VMEM(square, jnp.bfloat16) for _ in range(6)],
            pltpu.VMEM((2, 8, PANEL), jnp.float32),
            pltpu.SemaphoreType.DMA((len(partners) + 1,)),
            pltpu.SemaphoreType.DMA((2,)),
            pltpu.SemaphoreType.DMA,
            pltpu.SemaphoreType.DMA((max(len(partners) + 1, width // PANEL),)),
        ],
        input_output_aliases=aliases,
        compiler_params=pltpu.CompilerParams(vmem_limit_bytes=58 * 1024 * 1024),
        cost_estimate=pl.CostEstimate(flops=flops, bytes_accessed=20 * width * width, transcendentals=0),
    )(*operands)
    return results[0], results[1:-1], results[-1]


def gather_kernel(chunk, partners, me_ref, grad_hbm, *rest):
    count = len(partners)
    outs = rest[:count]
    squares_out, held, sem_in, sem_out = rest[count:]
    me = me_ref[0]
    loads = [
        pltpu.make_async_copy(grad_hbm.at[me ^ partner, chunk], held.at[n], sem_in.at[n])
        for n, partner in enumerate((*partners, 0))
    ]
    for load in loads:
        load.start()
    stores = []
    for n in range(count):
        loads[n].wait()
        store = pltpu.make_async_copy(held.at[n], outs[n], sem_out.at[n])
        store.start()
        stores.append(store)
    loads[count].wait()
    rows = 16

    def add_rows(i, total):
        at = pl.multiple_of(i * rows, rows)
        for n in range(count + 1):
            wide = held[n, pl.ds(at, rows), :].astype(jnp.float32)
            total = total + wide * wide
        return total

    width = held.shape[2]
    total = lax.fori_loop(0, held.shape[1] // rows, add_rows, jnp.zeros((rows, width), jnp.float32))
    squares_out[...] = jnp.broadcast_to(jnp.sum(total, keepdims=True), squares_out.shape)
    for store in stores:
        store.wait()


def gather_call(chunk, partners, me, by_owner):
    dev_rows, width = by_owner.shape[2:]
    hbm = pl.BlockSpec(memory_space=pltpu.HBM)
    count = len(partners)
    size = (count + 1) * dev_rows * width
    results = pl.pallas_call(
        functools.partial(gather_kernel, chunk, partners),
        out_shape=(
            *[jax.ShapeDtypeStruct((dev_rows, width), jnp.bfloat16) for _ in partners],
            jax.ShapeDtypeStruct((1, 128), jnp.float32),
        ),
        in_specs=[pl.BlockSpec(memory_space=pltpu.SMEM), hbm],
        out_specs=(*[hbm] * count, pl.BlockSpec(memory_space=pltpu.VMEM)),
        scratch_shapes=[
            pltpu.VMEM((count + 1, dev_rows, width), jnp.bfloat16),
            pltpu.SemaphoreType.DMA((count + 1,)),
            pltpu.SemaphoreType.DMA((count,)),
        ],
        compiler_params=pltpu.CompilerParams(vmem_limit_bytes=16 * 1024 * 1024),
        cost_estimate=pl.CostEstimate(flops=2 * size, bytes_accessed=4 * size, transcendentals=0),
    )(me, by_owner)
    return results[:-1], results[-1]


def scale_kernel(chunk, targets, me_ref, ratio_ref, *rest):
    pieces = rest[: len(targets)]
    out_ref, narrow, wide, sem_in, sem_out = rest[-5:]
    me = me_ref[0]
    if len(rest) < len(targets) + 5:
        pieces = [rest[0].at[n] for n in range(len(targets))]
    loads = [pltpu.make_async_copy(piece, narrow.at[n], sem_in.at[n]) for n, piece in enumerate(pieces)]
    for load in loads:
        load.start()
    stores = []
    for n, target in enumerate(targets):
        loads[n].wait()
        wide[n] = ratio_ref[0] * narrow[n].astype(jnp.float32)
        owner = n if target is None else me ^ target
        store = pltpu.make_async_copy(wide.at[n], out_ref.at[owner, chunk], sem_out.at[n])
        store.start()
        stores.append(store)
    for store in stores:
        store.wait()


def scale_call(chunk, out_shape, targets, me, ratio, pieces, carried):
    dev_rows, width = out_shape[2:]
    count = len(targets)
    hbm = pl.BlockSpec(memory_space=pltpu.HBM)
    smem = pl.BlockSpec(memory_space=pltpu.SMEM)
    operands = [me, ratio, *pieces]
    in_specs = [smem, smem] + [hbm] * len(pieces)
    aliases = {}
    if carried is not None:
        aliases = {len(operands): 0}
        operands.append(carried)
        in_specs.append(hbm)
    size = count * dev_rows * width
    return pl.pallas_call(
        functools.partial(scale_kernel, chunk, targets),
        out_shape=jax.ShapeDtypeStruct(out_shape, jnp.float32),
        in_specs=in_specs,
        out_specs=hbm,
        scratch_shapes=[
            pltpu.VMEM((count, dev_rows, width), jnp.bfloat16),
            pltpu.VMEM((count, dev_rows, width), jnp.float32),
            pltpu.SemaphoreType.DMA((count,)),
            pltpu.SemaphoreType.DMA((count,)),
        ],
        input_output_aliases=aliases,
        compiler_params=pltpu.CompilerParams(vmem_limit_bytes=16 * 1024 * 1024),
        cost_estimate=pl.CostEstimate(flops=size, bytes_accessed=6 * size, transcendentals=0),
    )(*operands)


def partner_order(owners):
    half = owners // 2
    order = (owners - 2, owners - 1, *range(2, half), *range(half, owners - 2), 1)
    return tuple(dict.fromkeys(d for d in order if 0 < d < owners))


def swap(piece, partner):
    size = lax.axis_size("dp")
    return lax.ppermute(piece, "dp", [(i, i ^ partner) for i in range(size)])


def sum_over(value, axis):
    size = lax.axis_size(axis)
    parts = [
        lax.ppermute(value, axis, [(i, (i + shift) % size) for i in range(size)])
        for shift in range(1, size)
    ]
    for part in parts:
        value = value + part
    return value


def exchange(pieces):
    return lax.all_to_all(pieces, "dp", split_axis=0, concat_axis=0, tiled=True)


def on_device(gradients, statistics, accumulator):
    owners = lax.axis_size("dp")
    row_blocks, col_blocks, dev_rows, block_width = gradients.shape
    blocks = row_blocks * col_blocks
    chunks = statistics.shape[1] // 2
    by_owner = gradients.reshape(owners, chunks, dev_rows, block_width)
    grads_wide = gradients.astype(jnp.float32)
    partners = partner_order(owners)
    me = lax.axis_index("dp").astype(jnp.int32).reshape(1)
    squares = jnp.zeros((1, 128), jnp.float32)
    received = []
    for c in range(chunks):
        pieces, part = gather_call(c, partners, me, by_owner)
        squares = squares + part
        parts = []
        for partner, piece in zip(partners, pieces):
            parts.append(swap(piece, partner))
        received.append(parts)
    grad_total = sum_over(squares, "mp")
    grad_total = sum_over(grad_total, "dp")[0, 0]
    entries = blocks * dev_rows * block_width * owners * lax.axis_size("mp")
    clip_factor = jnp.minimum(1.0, jnp.sqrt(entries / (grad_total + 1e-06)))
    scale = (0.1 / block_width * clip_factor * clip_factor).reshape(1)
    scaled = clip_factor * grads_wide
    accumulated = accumulator + scaled * scaled
    graft_step = scaled / jnp.sqrt(accumulated)
    graft_squares = jnp.sum(graft_step * graft_step)
    statistics_new = None
    returned = []
    update_squares = jnp.zeros((1, 128), jnp.float32)
    for c in range(chunks):
        whole = c + 1 < chunks
        statistics_new, product, part = block_call(
            c, partners, whole, me, scale, by_owner, received[c], statistics[0], statistics_new
        )
        update_squares = update_squares + part
        if whole:
            returned.append([exchange(product[0].reshape(owners, dev_rows, block_width))])
        else:
            parts = [product[0]]
            for n, partner in enumerate(partners):
                parts.append(swap(product[n + 1], partner))
            returned.append(parts)
    lanes = lax.broadcasted_iota(jnp.int32, (1, 128), 1)
    sums = jnp.where(lanes == 0, graft_squares, update_squares)
    sums = sum_over(sums, "mp")
    sums = sum_over(sums, "dp")
    graft_ratio = jnp.sqrt(sums[0, :1] / (sums[0, 1:2] + 1e-06))
    update = None
    out_shape = (owners, chunks, dev_rows, block_width)
    for c in range(chunks - 1):
        update = scale_call(c, out_shape, (None,) * owners, me, graft_ratio, returned[c], update)
    late = partners[-2]
    groups = (tuple(d for d in (0, *partners) if d != late), (late,))
    for group in groups:
        pieces = [dict(zip((0, *partners), returned[-1]))[d] for d in group]
        update = scale_call(chunks - 1, out_shape, group, me, graft_ratio, pieces, update)
    return (update.reshape(gradients.shape), statistics_new[None], accumulated)


def solution(mesh):
    def run(gradients, statistics, accumulator):
        if statistics.shape[1] != 4:
            return on_device_plain(gradients, statistics, accumulator)
        return on_device(gradients, statistics, accumulator)

    return jax.shard_map(
        run,
        mesh=mesh,
        in_specs=(P(None, "mp", "dp", None), P("mp", "dp", None, None), P(None, "mp", "dp", None)),
        out_specs=(P(None, "mp", "dp", None), P("mp", "dp", None, None), P(None, "mp", "dp", None)),
        check_vma=False,
    )
```
